32 devices in a mesh: rep: 2 (over core), ep: 16 (over z, y, x).
Axes of the slice: x: 2, y: 2, z: 4, core: 2. Of those that a mesh axis runs over, the one named last changes fastest.
Arguments:
- tokens: bfloat16 [4096, 2048], P(('rep', 'ep')), may hold values from -6 to 6
- gates: float32 [4096], P(('rep', 'ep')), may hold values from 0.25 to 1
- expert_ids: int32 [4096, 1], P(('rep', 'ep')), may hold values from 0 to 3; in each aligned block of 128 rows (0 to 127, 128 to 255, ...) at most 40 rows name the same one
- weight_in: bfloat16 [2048, 16384], P(None, 'ep'), may hold values from -0.125 to 0.125
- weight_out: bfloat16 [16384, 2048], P('ep'), may hold values from -0.09375 to 0.09375
Outputs:
- mixed: bfloat16 [4096, 2048], P(('rep', 'ep'))
The draws below stay inside these ranges and needn't reach their ends.
Inputs may be any that keep to these rules, and one draw needn't show every extreme that they name: `expert_ids`: among the 128 rows of one device no expert is named by more than 40 rows, and some expert is named by exactly that many in some devices' rows; every expert is named somewhere.
All inputs are finite; a program needn't handle non-finite values.
Results may differ from the reference program's by a relative error of at most 0.0057.
Values may be sent and summed in bfloat16 or wider, within the bound.
A program may use at most 64 MiB of HBM per device.

```python
import math
import jax
import jax.numpy as jnp
import numpy as np
from jax import lax

D = 2048
FF_DEV = 1024
SLICES = 4
FFW = 4096
EXPERTS = 4
TOK_DEV = 128
CAP = 24
OCAP = 16
TOKENS = 4096
DEVICES = 32


def block_scale(key, extent, cuts, smallest, largest):
    factor_of = 1.0
    for position, shards_of in cuts:
        steps = jax.random.uniform(jax.random.fold_in(jax.random.fold_in(key, 6), position), (shards_of,), jnp.float32, smallest / len(cuts), largest / len(cuts))
        factor_of = factor_of * jnp.repeat(jnp.exp(steps), extent[position] // shards_of).reshape((-1,) + (1,) * (len(extent) - 1 - position))
    return factor_of


def assign_block(stream_key, own, number, rows, count, top, bound, slope):
    order = jax.random.permutation(stream_key, count)
    packed, ordinary = portions_of(count, rows * top, bound, slope, True), portions_of(count, rows * top, bound, slope, False)
    places = jnp.arange(count)

    def named(lengths, rotation):
        used = int((lengths > 0).sum())
        fixed = max(1, used // 4)
        shifted = fixed + (places - fixed + rotation * (used - fixed)) % max(1, count - fixed)
        return jnp.zeros((count,), jnp.int32).at[order[jnp.where(places < fixed, places, shifted)]].set(jnp.asarray(lengths, jnp.int32))

    lengths = jnp.where(number % 4 == 0, named(packed, number // 4), named(ordinary, number - number // 4 - 1))
    mixed = jax.random.permutation(jax.random.fold_in(own, 3), count)
    source_of, receiver = mixed[0:count // 2 * 2:2], mixed[1:count // 2 * 2:2]
    slack = jnp.minimum(lengths[source_of] - 1, bound - lengths[receiver]) // 2
    slack = jnp.where((source_of == order[0]) | (receiver == order[0]) | (lengths[receiver] == 0), 0, jnp.maximum(slack, 0))
    shifted = jax.random.randint(jax.random.fold_in(own, 4), (count // 2,), 0, 1 << 20) % (slack + 1)
    lengths = lengths.at[source_of].add(-shifted).at[receiver].add(shifted)
    members = jnp.searchsorted(jnp.cumsum(lengths), jnp.arange(rows * top), side="right").astype(jnp.int32)
    grid = members.reshape(top, rows).T
    grid = grid[jax.random.permutation(jax.random.fold_in(own, 1), rows)]
    rotation = jax.random.randint(jax.random.fold_in(own, 2), (rows, 1), 0, top)
    return jnp.take_along_axis(grid, (jnp.arange(top)[None, :] + rotation) % top, axis=1)


def portions_of(number_of, total, reach, lean, full):
    portions = [(1 << 20) // math.isqrt(standing ** lean) + 1 for standing in range(1, number_of + 1)]
    largest = reach if full else min(reach, max(-(-total // number_of), total * portions[0] // sum(portions)))
    least = 1 if total - largest >= number_of - 1 else 0
    holding, spare = [largest] + [least] * (number_of - 1), total - largest - least * (number_of - 1)
    while spare > 0:
        free = [i for i in range(1, number_of) if holding[i] < largest] or [i for i in range(1, number_of) if holding[i] < reach]
        whole, left = sum([portions[i] for i in free]), spare
        for i in free:
            extra = min(reach - holding[i], max(1, left * portions[i] // whole), spare)
            holding[i] = holding[i] + extra
            spare = spare - extra
    return np.array(holding)


def gaussian(stream_key, extent, deviation, reach, shards=(), kind=jnp.bfloat16):
    level = block_scale(stream_key, extent, shards, -0.22, 0.18) if shards else 1.0
    values = jax.random.normal(stream_key, extent, jnp.float32) * deviation * level
    return jnp.minimum(jnp.maximum(values, -reach), reach).astype(kind)


def setup_inputs(seed: int = 0) -> dict:
    splits = jax.random.split(jax.random.key(seed), 6)
    tokens = gaussian(splits[0], (TOKENS, D), 1.0, 6.0, ((0, 32),))
    gates = jnp.clip(jnp.exp(math.log(1.0) - 1.3862944 * jax.random.uniform(splits[1], (TOKENS,), jnp.float32) ** block_scale(splits[1], (TOKENS,), ((0, 32),), -0.2, 0.2)), 0.25, 1.0)
    expert_ids_keys = jax.random.split(jax.random.fold_in(splits[2], 1), TOKENS // TOK_DEV)
    expert_ids_turns = jax.random.permutation(jax.random.fold_in(splits[2], 3), TOKENS // TOK_DEV)
    expert_ids = jax.vmap(lambda own, number: assign_block(jax.random.fold_in(splits[2], 2), own, number, TOK_DEV, EXPERTS, 1, CAP + OCAP, 2))(expert_ids_keys, expert_ids_turns).reshape((TOKENS, 1))
    weight_in = gaussian(splits[3], (D, EXPERTS * FFW), D ** -0.5, 0.125, ((1, 16),))
    weight_out = gaussian(splits[4], (EXPERTS * FFW, D), FFW ** -0.5, 0.09375, ((0, 16),))
    return {"tokens": tokens, "gates": gates, "expert_ids": expert_ids, "weight_in": weight_in, "weight_out": weight_out}


def reference(tokens, gates, expert_ids, weight_in, weight_out):
    expert_of = expert_ids[:, 0]
    total_rows = tokens.shape[0]
    width = tokens.shape[1]
    block_rows = DEVICES * (CAP + OCAP)
    order = jnp.argsort(expert_of, stable=True).astype(jnp.int32)
    ordered = tokens[order]
    padded = jnp.concatenate([ordered, jnp.zeros((block_rows, width), ordered.dtype)], axis=0)
    counts = jnp.sum((expert_of[:, None] == jnp.arange(EXPERTS, dtype=jnp.int32)[None, :]).astype(jnp.int32), axis=0)
    starts = (jnp.cumsum(counts) - counts).astype(jnp.int32)

    def serve(results, expert):
        start = starts[expert]
        block = lax.dynamic_slice_in_dim(padded, start, block_rows, 0)
        first = lax.dynamic_slice_in_dim(weight_in, expert * FFW, FFW, 1)
        second = lax.dynamic_slice_in_dim(weight_out, expert * FFW, FFW, 0)
        hidden = jnp.maximum(jnp.dot(block, first, preferred_element_type=jnp.float32), 0.0).astype(jnp.bfloat16)
        result = jnp.zeros((block_rows, width), jnp.float32)
        for piece in range(SLICES):
            partial_sum = jnp.dot(hidden[:, piece * FF_DEV:(piece + 1) * FF_DEV], second[piece * FF_DEV:(piece + 1) * FF_DEV, :], preferred_element_type=jnp.float32)
            rounded = lax.optimization_barrier(partial_sum.astype(jnp.bfloat16))
            result = result + rounded.astype(jnp.float32)
        valid = jnp.arange(block_rows, dtype=jnp.int32) < counts[expert]
        previous = lax.dynamic_slice_in_dim(results, start, block_rows, 0)
        merged = jnp.where(valid[:, None], result, previous)
        return lax.dynamic_update_slice_in_dim(results, merged, start, 0), 0

    initial = jnp.zeros((total_rows + block_rows, width), jnp.float32)
    results, unused = lax.scan(serve, initial, jnp.arange(EXPERTS, dtype=jnp.int32))
    expert_out = jnp.zeros((total_rows, width), jnp.float32).at[order].set(results[:total_rows])
    return (gates[:, None] * expert_out).astype(jnp.bfloat16)
```

```python
import functools

import jax
import jax.numpy as jnp
from jax import lax
from jax.experimental import pallas as pl
from jax.experimental.pallas import tpu as pltpu
from jax.sharding import PartitionSpec as P

SLICES = 4
CHUNKS = 4
STEP = 512
ORDER = (
    "a0c0t1Z1t2N2t3B0v2N3a1c1G0v3O3O2B1P0Q0a2c2",
    "B2G1P1a3c3Q1G2B3P2y2Q2x2E2G3P3Q3y3x3",
    "F2E3x1y1F3E1y0x0F1E0F0",
)
BF16 = jnp.bfloat16
F32 = jnp.float32
MESH = pl.DeviceIdType.MESH


def layout(owner_count, tok_rows):
    groups = owner_count // SLICES
    chunks = CHUNKS
    per = groups // chunks
    seats = 3 * tok_rows // (4 * groups) + tok_rows // (2 * groups)
    unit = 8 if per == 1 else 16
    seats = -(-seats // unit) * unit
    return groups, chunks, per, seats


def stack_rows(blocks):
    return jnp.concatenate([block.astype(F32) for block in blocks], axis=0).astype(BF16)


def flip(a, b, count):
    total, bit = 0, 1
    while bit < count:
        total = total + (a // bit % 2 + b // bit % 2) % 2 * bit
        bit *= 2
    return total


def kernel(
    owner_count,
    ids_hbm,
    gates_hbm,
    tokens_hbm,
    weight_in,
    weight_out,
    out,
    ids_row,
    gates,
    tokens,
    w_in,
    w_out,
    send,
    gathered,
    staged,
    hidden,
    parts,
    diag_a,
    diag_b,
    from_x,
    from_y,
    sums,
    returned,
    w_sem,
    z_send,
    z_recv,
    g_send,
    g_recv,
    r_send,
    r_recv,
    b_send,
    b_recv,
    far_sem,
):
    tok_rows, width = tokens.shape
    groups, chunks, per, seats = layout(owner_count, tok_rows)
    half = width // 2
    halves = (pl.ds(0, half), pl.ds(half, half))
    me = lax.axis_index("ep")
    group = me // SLICES
    lane = me % SLICES
    x_bit, y_bit = lane % 2, lane // 2
    x_lane = y_bit * 2 + (1 - x_bit)
    y_lane = (1 - y_bit) * 2 + x_bit
    d_lane = (1 - y_bit) * 2 + (1 - x_bit)
    x_dev = group * SLICES + x_lane
    y_dev = group * SLICES + y_lane
    inner = (group % 2 + group // 2 % 2) % 2
    chunk_of = [0, 1, 2 + inner, 3 - inner]

    barrier = pltpu.get_barrier_semaphore()
    pl.semaphore_signal(barrier, inc=1, device_id={"ep": x_dev}, device_id_type=MESH)
    pl.semaphore_signal(barrier, inc=1, device_id={"ep": y_dev}, device_id_type=MESH)
    near = groups == 4

    def greet(sem, k):
        other = flip(group, k, groups) * SLICES + lane
        pl.semaphore_signal(sem, inc=1, device_id={"ep": other}, device_id_type=MESH)

    if near:
        greet(barrier, 1)
        pl.when(inner == 1)(lambda: greet(barrier, 3))
        greeted = 3 + inner
    else:
        for k in range(1, groups):
            greet(barrier, k)
        greeted = 2 + groups - 1

    load_ids = pltpu.make_async_copy(ids_hbm, ids_row, w_sem.at[2])
    load_gates = pltpu.make_async_copy(gates_hbm, gates, w_sem.at[3])
    load_tokens = pltpu.make_async_copy(tokens_hbm, tokens, w_sem.at[4])
    load_in = pltpu.make_async_copy(weight_in, w_in, w_sem.at[0])
    load_out = pltpu.make_async_copy(weight_out, w_out, w_sem.at[1])
    for load in (load_ids, load_gates, load_tokens, load_in, load_out):
        load.start()

    lanes_e = -(-groups // 16) * 16
    t0 = lax.broadcasted_iota(jnp.int32, (tok_rows, tok_rows), 0)
    t1 = lax.broadcasted_iota(jnp.int32, (tok_rows, tok_rows), 1)
    load_ids.wait()
    ids = ids_row[...]
    hot = (lax.broadcasted_iota(jnp.int32, (lanes_e, tok_rows), 0) == ids).astype(F32)
    ahead = jnp.dot(hot.astype(BF16), (t0 < t1).astype(F32).astype(BF16), preferred_element_type=F32)
    slot = ids * seats + jnp.sum(hot * ahead, axis=0, keepdims=True).astype(jnp.int32)
    load_gates.wait()
    slot_c = jnp.sum(jnp.where(t0 == t1, slot, 0), axis=1, keepdims=True)
    weight = jnp.sum(jnp.where(t0 == t1, gates[...], 0.0), axis=1, keepdims=True)
    load_tokens.wait()

    def take(target, dst):
        seat = lax.broadcasted_iota(jnp.int32, (seats, tok_rows), 0) + target * seats
        place = (seat == slot).astype(F32).astype(BF16)
        for c in range(0, width, STEP):
            rows = jnp.dot(place, tokens[:, c : c + STEP], preferred_element_type=F32)
            dst[:, c : c + STEP] = rows.astype(BF16)

    def remote(src, dst, s_sem, r_sem, dev):
        return pltpu.make_async_remote_copy(
            src_ref=src,
            dst_ref=dst,
            send_sem=s_sem,
            recv_sem=r_sem,
            device_id={"ep": dev},
            device_id_type=MESH,
        )

    def seat_rows(ref, i):
        return ref.at[pl.ds(i * seats, seats)] if per > 1 else ref

    members = [(p, i) for p in range(chunks) for i in range(per)][1:]
    spread, forward, early, late, z_copies, back = {}, {}, {}, {}, {}, {}

    def take_for(p, i):
        k = chunk_of[p] * per + i
        target = flip(group, k, groups)
        source = send.at[p * per + i]
        landing = seat_rows(gathered.at[chunk_of[p], lane], i)
        take(target, source)
        z_copies[p, i] = [
            remote(
                source.at[:, cols],
                landing.at[:, cols],
                z_send.at[k, h],
                z_recv.at[k, h],
                target * SLICES + lane,
            )
            for h, cols in enumerate(halves)
        ]

    def stage_t(p):
        if per == 1:
            take_for(p, 0)

    def leave(p):
        for i in range(per):
            if (p, i) in z_copies:
                for copy in z_copies[p, i]:
                    copy.start()

    def stage_z(p):
        leave(p)

    def stage_n(p):
        pl.when(inner == 1)(lambda: leave(p))

    def stage_o(p):
        pl.when(inner == 0)(lambda: leave(p))

    def stage_v(p):
        if near and p == 2:
            pl.semaphore_wait(far_sem.at[0], 1)
            pl.when(inner == 1)(lambda: greet(far_sem.at[1], 1))
        if near and p == 3:
            pl.when(inner == 0)(lambda: pl.semaphore_wait(far_sem.at[1], 1))

    def stage_a(p):
        own = [gathered.at[chunk_of[p], lane, :, cols] for cols in halves]

        def arrive(h):
            for i in range(per):
                if (p, i) in z_copies:
                    z_copies[p, i][h].wait_recv()

        spread[p] = [
            remote(own[h], own[h], g_send.at[p, n], g_recv.at[p, n], dev)
            for n, (h, dev) in enumerate(((0, x_dev), (1, y_dev), (1, x_dev), (0, y_dev)))
        ]
        arrive(0)
        spread[p][0].start()
        arrive(1)
        spread[p][1].start()

    def stage_c(p):
        for copy in spread[p][2:]:
            copy.start()

    def stage_b(p):
        first = gathered.at[chunk_of[p], x_lane, :, halves[0]]
        second = gathered.at[chunk_of[p], y_lane, :, halves[1]]
        forward[p] = [
            remote(first, first, g_send.at[p, 4], g_recv.at[p, 4], y_dev),
            remote(second, second, g_send.at[p, 5], g_recv.at[p, 5], x_dev),
        ]
        for arrived, onward in zip(spread[p], forward[p]):
            arrived.wait_recv()
            onward.start()

    rows = per * seats
    tile = STEP

    def stage_g(p):
        for copy in spread[p][2:] + forward[p]:
            copy.wait_recv()
        staged[...] = stack_rows([gathered[chunk_of[p], s] for s in range(SLICES)])
        if p == 0:
            load_in.wait()

        @pl.loop(0, w_in.shape[1] // tile)
        def _(n):
            cols = pl.ds(pl.multiple_of(n * tile, tile), tile)
            value = jnp.dot(staged[...], w_in[:, cols], preferred_element_type=F32)
            hidden[:, cols] = jnp.maximum(value, 0.0).astype(BF16)

        if p == 0:
            load_out.wait()

    def project(p, start):
        @pl.loop(0, half // tile)
        def _(n):
            cols = pl.ds(pl.multiple_of(start + n * tile, tile), tile)
            value = jnp.dot(hidden[...], w_out[:, cols], preferred_element_type=F32)
            for s in range(SLICES):
                parts[p, s, :, cols] = value[s * rows : (s + 1) * rows].astype(BF16)

    def stage_p(p):
        project(p, 0)

    def stage_q(p):
        project(p, half)

    def to(p, n, src, dst, dev):
        return remote(src, dst, r_send.at[p, n], r_recv.at[p, n], dev)

    def stage_y(p):
        early[p, 0] = to(p, 0, parts.at[p, d_lane, :, halves[0]], diag_a.at[p], y_dev)
        early[p, 1] = to(
            p, 1, parts.at[p, y_lane, :, halves[0]], from_y.at[p, :, halves[0]], y_dev
        )
        early[p, 0].start()
        early[p, 1].start()

    def stage_x(p):
        early[p, 2] = to(p, 2, parts.at[p, d_lane, :, halves[1]], diag_b.at[p], x_dev)
        early[p, 3] = to(
            p, 3, parts.at[p, x_lane, :, halves[1]], from_x.at[p, :, halves[1]], x_dev
        )
        early[p, 2].start()
        early[p, 3].start()

    def stage_e(p):
        late[p] = [
            to(p, 4, parts.at[p, x_lane, :, halves[0]], from_x.at[p, :, halves[0]], x_dev),
            to(p, 5, parts.at[p, y_lane, :, halves[1]], from_y.at[p, :, halves[1]], y_dev),
        ]
        early[p, 0].wait_recv()
        parts[p, x_lane, :, :half] = (
            parts[p, x_lane, :, :half].astype(F32) + diag_a[p].astype(F32)
        ).astype(BF16)
        late[p][0].start()
        early[p, 2].wait_recv()
        parts[p, y_lane, :, half:] = (
            parts[p, y_lane, :, half:].astype(F32) + diag_b[p].astype(F32)
        ).astype(BF16)
        late[p][1].start()

    def stage_f(p):
        for h, cols in enumerate((slice(0, half), slice(half, width))):
            for copy in (late[p][h], early[p, 1 + 2 * h]):
                copy.wait_recv()
            sums[p, :, cols] = (
                parts[p, lane, :, cols].astype(F32)
                + from_x[p, :, cols].astype(F32)
                + from_y[p, :, cols].astype(F32)
            ).astype(BF16)
            for i in range(per):
                if (p, i) in z_copies:
                    k = chunk_of[p] * per + i
                    back[p, i, h] = remote(
                        seat_rows(sums.at[p], i).at[:, halves[h]],
                        returned.at[k, :, halves[h]],
                        b_send.at[k, h],
                        b_recv.at[k, h],
                        flip(group, k, groups) * SLICES + lane,
                    )
                    back[p, i, h].start()

    take(group, seat_rows(gathered.at[0, lane], 0))
    if per > 1:
        for p, i in members:
            take_for(p, i)
    pl.semaphore_wait(barrier, greeted)
    if near:

        @pl.when(inner == 1)
        def _():
            greet(far_sem.at[0], 1)
            greet(far_sem.at[0], 3)

    if per > 1:
        leave(0)

    stages = {
        "a": stage_a,
        "c": stage_c,
        "t": stage_t,
        "v": stage_v,
        "Z": stage_z,
        "N": stage_n,
        "O": stage_o,
        "B": stage_b,
        "G": stage_g,
        "P": stage_p,
        "Q": stage_q,
        "y": stage_y,
        "x": stage_x,
        "E": stage_e,
        "F": stage_f,
    }
    order = "".join(ORDER)
    for name, p in zip(order[::2], order[1::2]):
        stages[name](int(p))

    picks = []
    for p in range(chunks):
        for i in range(per):
            target = flip(group, chunk_of[p] * per + i, groups)
            seat = lax.broadcasted_iota(jnp.int32, (tok_rows, seats), 1) + target * seats
            picks.append((seat == slot_c).astype(F32))
    pick = jnp.concatenate(picks, axis=1).astype(BF16)
    for h in range(2):
        for p, i in members:
            back[p, i, h].wait_recv()
        for c in range(h * half, (h + 1) * half, STEP):
            blocks = [sums[0, :seats, c : c + STEP]]
            blocks += [returned[chunk_of[p] * per + i, :, c : c + STEP] for p, i in members]
            picked = jnp.dot(pick, stack_rows(blocks), preferred_element_type=F32)
            out[:, c : c + STEP] = (weight * picked).astype(BF16)

    for p in range(chunks):
        for copy in spread[p] + forward[p] + late[p] + [early[p, n] for n in range(4)]:
            copy.wait_send()
    for p, i in members:
        for h in range(2):
            z_copies[p, i][h].wait_send()
            back[p, i, h].wait_send()


def body(tokens, gates, expert_ids, weight_in, weight_out):
    owner_count = lax.axis_size("ep")
    tok_rows, width = tokens.shape
    groups, chunks, per, seats = layout(owner_count, tok_rows)
    rows = per * seats
    half = width // 2
    hbm = pl.BlockSpec(memory_space=pltpu.HBM)
    dma = pltpu.SemaphoreType.DMA
    return pl.pallas_call(
        functools.partial(kernel, owner_count),
        out_shape=jax.ShapeDtypeStruct((tok_rows, width), BF16),
        in_specs=[hbm] * 5,
        out_specs=pl.BlockSpec(memory_space=pltpu.VMEM),
        scratch_shapes=[
            pltpu.VMEM((1, tok_rows), jnp.int32),
            pltpu.VMEM((1, tok_rows), F32),
            pltpu.VMEM((tok_rows, width), BF16),
            pltpu.VMEM(weight_in.shape, BF16),
            pltpu.VMEM(weight_out.shape, BF16),
            pltpu.VMEM((groups, seats, width), BF16),
            pltpu.VMEM((chunks, SLICES, rows, width), BF16),
            pltpu.VMEM((SLICES * rows, width), BF16),
            pltpu.VMEM((SLICES * rows, weight_in.shape[1]), BF16),
            pltpu.VMEM((chunks, SLICES, rows, width), BF16),
            pltpu.VMEM((chunks, rows, half), BF16),
            pltpu.VMEM((chunks, rows, half), BF16),
            pltpu.VMEM((chunks, rows, width), BF16),
            pltpu.VMEM((chunks, rows, width), BF16),
            pltpu.VMEM((chunks, rows, width), BF16),
            pltpu.VMEM((groups, seats, width), BF16),
            dma((5,)),
            dma((groups, 2)),
            dma((groups, 2)),
            dma((chunks, 6)),
            dma((chunks, 6)),
            dma((chunks, 6)),
            dma((chunks, 6)),
            dma((groups, 2)),
            dma((groups, 2)),
            pltpu.SemaphoreType.REGULAR((2,)),
        ],
        compiler_params=pltpu.CompilerParams(
            collective_id=0, has_side_effects=True, vmem_limit_bytes=48 * 1024 * 1024
        ),
    )(
        *(
            pltpu.with_memory_space_constraint(array, pltpu.HBM)
            for array in (
                expert_ids.reshape(1, tok_rows),
                gates.reshape(1, tok_rows),
                tokens,
                weight_in,
                weight_out,
            )
        )
    )


def solution(mesh):
    in_specs = (
        P(("rep", "ep"), None),
        P(("rep", "ep")),
        P(("rep", "ep"), None),
        P(None, "ep"),
        P("ep", None),
    )
    out_specs = P(("rep", "ep"), None)
    return jax.shard_map(body, mesh=mesh, in_specs=in_specs, out_specs=out_specs, check_vma=False)
```

```python
import functools

import jax
import jax.numpy as jnp
from jax import lax
from jax.experimental import pallas as pl
from jax.experimental.pallas import tpu as pltpu
from jax.sharding import PartitionSpec as P

SLICES = 4
CHUNKS = 4
STEP = 512
ORDER = (
    "a0c0t1Z1t2N2C0B0t3u2N3a1c1G0B1C1u3O3P0O2Q0a2c2G1P1C2B2Q1a3c3",
    "G2x1w1P2B3C3y1Q2x2G3P3E1y3Q3x3H2y2v2E3w3H3w2v3F1I2E2x0y0v1F3",
    "H1w0v0I3F2H0E0I1R0F0S0I0T0",
)
BF16 = jnp.bfloat16
F32 = jnp.float32
MESH = pl.DeviceIdType.MESH


def layout(owner_count, tok_rows):
    groups = owner_count // SLICES
    chunks = CHUNKS
    per = groups // chunks
    seats = 3 * tok_rows // (4 * groups) + tok_rows // (2 * groups)
    unit = 8 if per == 1 else 16
    seats = -(-seats // unit) * unit
    return groups, chunks, per, seats


def stack_rows(blocks):
    return jnp.concatenate([block.astype(F32) for block in blocks], axis=0).astype(BF16)


def flip(a, b, count):
    total, bit = 0, 1
    while bit < count:
        total = total + (a // bit % 2 + b // bit % 2) % 2 * bit
        bit *= 2
    return total


def kernel(
    owner_count,
    ids_hbm,
    gates_hbm,
    tokens_hbm,
    weight_in,
    weight_out,
    out,
    ids_row,
    gates,
    tokens,
    w_in,
    w_out,
    send,
    gathered,
    staged,
    hidden,
    parts,
    diag_a,
    diag_b,
    from_x,
    from_y,
    sums,
    returned,
    total,
    w_sem,
    z_send,
    z_recv,
    g_send,
    g_recv,
    r_send,
    r_recv,
    b_send,
    b_recv,
    far_sem,
):
    tok_rows, width = tokens.shape
    groups, chunks, per, seats = layout(owner_count, tok_rows)
    half = width // 2
    halves = (pl.ds(0, half), pl.ds(half, half))
    me = lax.axis_index("ep")
    group = me // SLICES
    lane = me % SLICES
    x_bit, y_bit = lane % 2, lane // 2
    x_lane = y_bit * 2 + (1 - x_bit)
    y_lane = (1 - y_bit) * 2 + x_bit
    d_lane = (1 - y_bit) * 2 + (1 - x_bit)
    x_dev = group * SLICES + x_lane
    y_dev = group * SLICES + y_lane
    inner = (group % 2 + group // 2 % 2) % 2
    chunk_of = [0, 1, 2 + inner, 3 - inner]

    barrier = pltpu.get_barrier_semaphore()
    pl.semaphore_signal(barrier, inc=1, device_id={"ep": x_dev}, device_id_type=MESH)
    pl.semaphore_signal(barrier, inc=1, device_id={"ep": y_dev}, device_id_type=MESH)
    near = groups == 4

    def greet(sem, k):
        other = flip(group, k, groups) * SLICES + lane
        pl.semaphore_signal(sem, inc=1, device_id={"ep": other}, device_id_type=MESH)

    if near:
        greet(barrier, 1)
        pl.when(inner == 1)(lambda: greet(barrier, 3))
        greeted = 3 + inner
    else:
        for k in range(1, groups):
            greet(barrier, k)
        greeted = 2 + groups - 1

    load_ids = pltpu.make_async_copy(ids_hbm, ids_row, w_sem.at[2])
    load_gates = pltpu.make_async_copy(gates_hbm, gates, w_sem.at[3])
    load_tokens = pltpu.make_async_copy(tokens_hbm, tokens, w_sem.at[4])
    load_in = pltpu.make_async_copy(weight_in, w_in, w_sem.at[0])
    load_out = pltpu.make_async_copy(weight_out, w_out, w_sem.at[1])
    for load in (load_ids, load_gates, load_tokens, load_in, load_out):
        load.start()

    lanes_e = -(-groups // 16) * 16
    t0 = lax.broadcasted_iota(jnp.int32, (tok_rows, tok_rows), 0)
    t1 = lax.broadcasted_iota(jnp.int32, (tok_rows, tok_rows), 1)
    load_ids.wait()
    ids = ids_row[...]
    hot = (lax.broadcasted_iota(jnp.int32, (lanes_e, tok_rows), 0) == ids).astype(F32)
    ahead = jnp.dot(hot.astype(BF16), (t0 < t1).astype(F32).astype(BF16), preferred_element_type=F32)
    slot = ids * seats + jnp.sum(hot * ahead, axis=0, keepdims=True).astype(jnp.int32)
    load_gates.wait()
    slot_c = jnp.sum(jnp.where(t0 == t1, slot, 0), axis=1, keepdims=True)
    weight = jnp.sum(jnp.where(t0 == t1, gates[...], 0.0), axis=1, keepdims=True)
    load_tokens.wait()

    def take(target, dst):
        seat = lax.broadcasted_iota(jnp.int32, (seats, tok_rows), 0) + target * seats
        place = (seat == slot).astype(F32).astype(BF16)
        for c in range(0, width, STEP):
            rows = jnp.dot(place, tokens[:, c : c + STEP], preferred_element_type=F32)
            dst[:, c : c + STEP] = rows.astype(BF16)

    def remote(src, dst, s_sem, r_sem, dev):
        return pltpu.make_async_remote_copy(
            src_ref=src,
            dst_ref=dst,
            send_sem=s_sem,
            recv_sem=r_sem,
            device_id={"ep": dev},
            device_id_type=MESH,
        )

    def drain(ref, sem):
        pltpu.make_async_copy(ref, ref, sem).wait()

    def seat_rows(ref, i):
        return ref.at[pl.ds(i * seats, seats)] if per > 1 else ref

    members = [(p, i) for p in range(chunks) for i in range(per)][1:]
    spread, forward, early, late, z_copies, back = {}, {}, {}, {}, {}, {}

    def take_for(p, i):
        k = chunk_of[p] * per + i
        target = flip(group, k, groups)
        source = send.at[p * per + i]
        landing = seat_rows(gathered.at[chunk_of[p], lane], i)
        take(target, source)
        z_copies[p, i] = [
            remote(
                source.at[:, cols],
                landing.at[:, cols],
                z_send,
                z_recv.at[k - 1, h],
                target * SLICES + lane,
            )
            for h, cols in enumerate(halves)
        ]

    def stage_t(p):
        if per == 1:
            take_for(p, 0)

    def leave(p):
        for i in range(per):
            if (p, i) in z_copies:
                for copy in z_copies[p, i]:
                    copy.start()

    def stage_z(p):
        leave(p)

    def stage_n(p):
        pl.when(inner == 1)(lambda: leave(p))

    def stage_o(p):
        pl.when(inner == 0)(lambda: leave(p))

    def stage_u(p):
        if near and p == 2:
            pl.semaphore_wait(far_sem.at[0], 1)
            pl.when(inner == 1)(lambda: greet(far_sem.at[1], 1))
        if near and p == 3:
            pl.when(inner == 0)(lambda: pl.semaphore_wait(far_sem.at[1], 1))

    def stage_a(p):
        own = [gathered.at[chunk_of[p], lane, :, cols] for cols in halves]

        def arrive(h):
            for i in range(per):
                if (p, i) in z_copies:
                    z_copies[p, i][h].wait_recv()

        spread[p] = [
            remote(own[h], own[h], g_send, g_recv.at[p, n], dev)
            for n, h, dev in ((0, 0, x_dev), (1, 1, y_dev), (2, 1, x_dev), (2, 0, y_dev))
        ]
        first = gathered.at[chunk_of[p], x_lane, :, halves[0]]
        second = gathered.at[chunk_of[p], y_lane, :, halves[1]]
        forward[p] = [
            remote(first, first, g_send, g_recv.at[p, 2], y_dev),
            remote(second, second, g_send, g_recv.at[p, 2], x_dev),
        ]
        arrive(0)
        spread[p][0].start()
        arrive(1)
        spread[p][1].start()

    def stage_c(p):
        for copy in spread[p][2:]:
            copy.start()

    def stage_b(p):
        spread[p][0].wait_recv()
        forward[p][0].start()

    def stage_k(p):
        spread[p][1].wait_recv()
        forward[p][1].start()

    rows = per * seats
    tile = STEP

    def stage_g(p):
        drain(gathered.at[chunk_of[p], pl.ds(0, 2)], g_recv.at[p, 2])
        staged[...] = stack_rows([gathered[chunk_of[p], s] for s in range(SLICES)])
        if p == 0:
            load_in.wait()

        @pl.loop(0, w_in.shape[1] // tile)
        def _(n):
            cols = pl.ds(pl.multiple_of(n * tile, tile), tile)
            value = jnp.dot(staged[...], w_in[:, cols], preferred_element_type=F32)
            hidden[:, cols] = jnp.maximum(value, 0.0).astype(BF16)

        if p == 0:
            load_out.wait()

    def project(p, start):
        @pl.loop(0, half // tile)
        def _(n):
            cols = pl.ds(pl.multiple_of(start + n * tile, tile), tile)
            value = jnp.dot(hidden[...], w_out[:, cols], preferred_element_type=F32)
            for s in range(SLICES):
                parts[p, s, :, cols] = value[s * rows : (s + 1) * rows].astype(BF16)

    def stage_p(p):
        project(p, 0)

    def stage_q(p):
        project(p, half)

    def to(p, n, src, dst, dev):
        return remote(src, dst, r_send, r_recv.at[p, n], dev)

    def stage_y(p):
        early[p, 0] = to(p, 0, parts.at[p, d_lane, :, halves[0]], diag_a.at[p], y_dev)
        early[p, 0].start()

    def stage_w(p):
        early[p, 1] = to(
            p, 2, parts.at[p, y_lane, :, halves[0]], from_y.at[p, :, halves[0]], y_dev
        )
        early[p, 1].start()

    def stage_x(p):
        early[p, 2] = to(p, 1, parts.at[p, d_lane, :, halves[1]], diag_b.at[p], x_dev)
        early[p, 2].start()

    def stage_v(p):
        early[p, 3] = to(
            p, 3, parts.at[p, x_lane, :, halves[1]], from_x.at[p, :, halves[1]], x_dev
        )
        early[p, 3].start()

    def stage_e(p):
        late[p, 0] = to(p, 2, parts.at[p, x_lane, :, halves[0]], from_x.at[p, :, halves[0]], x_dev)
        early[p, 0].wait_recv()
        parts[p, x_lane, :, :half] = (
            parts[p, x_lane, :, :half].astype(F32) + diag_a[p].astype(F32)
        ).astype(BF16)
        late[p, 0].start()

    def stage_h(p):
        late[p, 1] = to(p, 3, parts.at[p, y_lane, :, halves[1]], from_y.at[p, :, halves[1]], y_dev)
        early[p, 2].wait_recv()
        parts[p, y_lane, :, half:] = (
            parts[p, y_lane, :, half:].astype(F32) + diag_b[p].astype(F32)
        ).astype(BF16)
        late[p, 1].start()

    def finish(p, h):
        cols = slice(h * half, (h + 1) * half)
        drain(from_x.at[p], r_recv.at[p, 2 + h])
        sums[p, :, cols] = (
            parts[p, lane, :, cols].astype(F32)
            + from_x[p, :, cols].astype(F32)
            + from_y[p, :, cols].astype(F32)
        ).astype(BF16)
        for i in range(per):
            if (p, i) in z_copies:
                k = chunk_of[p] * per + i
                back[p, i, h] = remote(
                    seat_rows(sums.at[p], i).at[:, halves[h]],
                    returned.at[k, :, halves[h]],
                    b_send,
                    b_recv.at[0 if p > 0 else 1 + h],
                    flip(group, k, groups) * SLICES + lane,
                )
                back[p, i, h].start()

    def stage_f(p):
        finish(p, 0)

    def stage_i(p):
        finish(p, 1)

    def picks_of(wanted):
        picks = []
        for p, i in wanted:
            target = flip(group, chunk_of[p] * per + i, groups)
            seat = lax.broadcasted_iota(jnp.int32, (tok_rows, seats), 1) + target * seats
            picks.append((seat == slot_c).astype(F32))
        return jnp.concatenate(picks, axis=1).astype(BF16)

    def gather(wanted, h, c):
        blocks = []
        for q, i in wanted:
            if (q, i) == (0, 0):
                blocks.append(sums[0, :seats, c : c + STEP])
            else:
                blocks.append(returned[chunk_of[q] * per + i, :, c : c + STEP])
        return jnp.dot(picks_of(wanted), stack_rows(blocks), preferred_element_type=F32)

    def stage_r(p):
        wanted = [(q, i) for q, i in members if q > 0]
        drain(returned.at[pl.ds(0, len(wanted))], b_recv.at[0])
        for h in range(2):
            for c in range(h * half, (h + 1) * half, STEP):
                total[:, c : c + STEP] = gather(wanted, h, c)

    def store(h):
        if per > 1:
            drain(returned.at[pl.ds(0, per - 1), :, halves[h]], b_recv.at[1 + h])
        wanted = [(0, i) for i in range(per)]
        for c in range(h * half, (h + 1) * half, STEP):
            picked = total[:, c : c + STEP] + gather(wanted, h, c)
            out[:, c : c + STEP] = (weight * picked).astype(BF16)

    def stage_s(p):
        store(0)

    def stage_j(p):
        store(1)

    take(group, seat_rows(gathered.at[0, lane], 0))
    if per > 1:
        for p, i in members:
            take_for(p, i)
    pl.semaphore_wait(barrier, greeted)
    if near:

        @pl.when(inner == 1)
        def _():
            greet(far_sem.at[0], 1)
            greet(far_sem.at[0], 3)

    if per > 1:
        leave(0)

    stages = {
        "a": stage_a,
        "c": stage_c,
        "t": stage_t,
        "u": stage_u,
        "Z": stage_z,
        "N": stage_n,
        "O": stage_o,
        "B": stage_b,
        "C": stage_k,
        "G": stage_g,
        "P": stage_p,
        "Q": stage_q,
        "y": stage_y,
        "w": stage_w,
        "x": stage_x,
        "v": stage_v,
        "E": stage_e,
        "H": stage_h,
        "F": stage_f,
        "I": stage_i,
        "R": stage_r,
        "S": stage_s,
        "T": stage_j,
    }
    order = "".join(ORDER)
    for name, p in zip(order[::2], order[1::2]):
        stages[name](int(p))

    drain(send.at[pl.ds(0, len(members))], z_send)
    drain(parts.at[pl.ds(0, 3)], g_send)
    drain(parts.at[pl.ds(0, 3)], r_send)
    drain(returned.at[pl.ds(0, len(members))], b_send)


def body(tokens, gates, expert_ids, weight_in, weight_out):
    owner_count = lax.axis_size("ep")
    tok_rows, width = tokens.shape
    groups, chunks, per, seats = layout(owner_count, tok_rows)
    rows = per * seats
    half = width // 2
    hbm = pl.BlockSpec(memory_space=pltpu.HBM)
    dma = pltpu.SemaphoreType.DMA
    return pl.pallas_call(
        functools.partial(kernel, owner_count),
        out_shape=jax.ShapeDtypeStruct((tok_rows, width), BF16),
        in_specs=[hbm] * 5,
        out_specs=pl.BlockSpec(memory_space=pltpu.VMEM),
        scratch_shapes=[
            pltpu.VMEM((1, tok_rows), jnp.int32),
            pltpu.VMEM((1, tok_rows), F32),
            pltpu.VMEM((tok_rows, width), BF16),
            pltpu.VMEM(weight_in.shape, BF16),
            pltpu.VMEM(weight_out.shape, BF16),
            pltpu.VMEM((groups, seats, width), BF16),
            pltpu.VMEM((chunks, SLICES, rows, width), BF16),
            pltpu.VMEM((SLICES * rows, width), BF16),
            pltpu.VMEM((SLICES * rows, weight_in.shape[1]), BF16),
            pltpu.VMEM((chunks, SLICES, rows, width), BF16),
            pltpu.VMEM((chunks, rows, half), BF16),
            pltpu.VMEM((chunks, rows, half), BF16),
            pltpu.VMEM((chunks, rows, width), BF16),
            pltpu.VMEM((chunks, rows, width), BF16),
            pltpu.VMEM((chunks, rows, width), BF16),
            pltpu.VMEM((groups, seats, width), BF16),
            pltpu.VMEM((tok_rows, width), F32),
            dma((5,)),
            dma,
            dma((groups - 1, 2)),
            dma,
            dma((chunks, 3)),
            dma,
            dma((chunks, 4)),
            dma,
            dma((3,)),
            pltpu.SemaphoreType.REGULAR((2,)),
        ],
        compiler_params=pltpu.CompilerParams(
            collective_id=0, has_side_effects=True, vmem_limit_bytes=48 * 1024 * 1024
        ),
    )(
        *(
            pltpu.with_memory_space_constraint(array, pltpu.HBM)
            for array in (
                expert_ids.reshape(1, tok_rows),
                gates.reshape(1, tok_rows),
                tokens,
                weight_in,
                weight_out,
            )
        )
    )


def solution(mesh):
    in_specs = (
        P(("rep", "ep"), None),
        P(("rep", "ep")),
        P(("rep", "ep"), None),
        P(None, "ep"),
        P("ep", None),
    )
    out_specs = P(("rep", "ep"), None)
    return jax.shard_map(body, mesh=mesh, in_specs=in_specs, out_specs=out_specs, check_vma=False)
```

```python
import functools

import jax
import jax.numpy as jnp
from jax import lax
from jax.experimental import pallas as pl
from jax.experimental.pallas import tpu as pltpu
from jax.sharding import PartitionSpec as P

SLICES = 4
CHUNKS = 4
STEP = 512
ORDER = (
    "a0c0t1Z1t2N2C0B0t3u2N3a1c1G0B1C1u3O3P0O2Q0a2c2G1P1C2B2Q1a3c3",
    "G2x1w1P2C3B3y1Q2x2G3P3E1y3Q3x3H2y2v2E3w3H3w2v3F1I2E2x0y0v1F3",
    "H1v0I3F2H0w0E0I1R3F0I0S2T1",
)
OTHER = ORDER
BF16 = jnp.bfloat16
F32 = jnp.float32
MESH = pl.DeviceIdType.MESH


def layout(owner_count, tok_rows):
    groups = owner_count // SLICES
    chunks = CHUNKS
    per = groups // chunks
    seats = 3 * tok_rows // (4 * groups) + tok_rows // (2 * groups)
    unit = 8 if per == 1 else 16
    seats = -(-seats // unit) * unit
    return groups, chunks, per, seats


def stack_rows(blocks):
    return jnp.concatenate([block.astype(F32) for block in blocks], axis=0).astype(BF16)


def flip(a, b, count):
    total, bit = 0, 1
    while bit < count:
        total = total + (a // bit % 2 + b // bit % 2) % 2 * bit
        bit *= 2
    return total


def kernel(
    owner_count,
    ids_hbm,
    gates_hbm,
    tokens_hbm,
    weight_in,
    weight_out,
    out,
    ids_row,
    gates,
    tokens,
    w_in,
    w_out,
    send,
    gathered,
    staged,
    hidden,
    parts,
    diag_a,
    diag_b,
    from_x,
    from_y,
    sums,
    returned,
    total,
    w_sem,
    z_send,
    z_recv,
    g_send,
    g_recv,
    r_send,
    r_recv,
    b_send,
    b_recv,
    far_sem,
):
    tok_rows, width = tokens.shape
    groups, chunks, per, seats = layout(owner_count, tok_rows)
    half = width // 2
    halves = (pl.ds(0, half), pl.ds(half, half))
    me = lax.axis_index("ep")
    group = me // SLICES
    lane = me % SLICES
    x_bit, y_bit = lane % 2, lane // 2
    x_lane = y_bit * 2 + (1 - x_bit)
    y_lane = (1 - y_bit) * 2 + x_bit
    d_lane = (1 - y_bit) * 2 + (1 - x_bit)
    x_dev = group * SLICES + x_lane
    y_dev = group * SLICES + y_lane
    inner = (group % 2 + group // 2 % 2) % 2
    chunk_of = [0, 1, 2 + inner, 3 - inner]

    barrier = pltpu.get_barrier_semaphore()
    pl.semaphore_signal(barrier, inc=1, device_id={"ep": x_dev}, device_id_type=MESH)
    pl.semaphore_signal(barrier, inc=1, device_id={"ep": y_dev}, device_id_type=MESH)
    near = groups == 4

    def greet(sem, k):
        other = flip(group, k, groups) * SLICES + lane
        pl.semaphore_signal(sem, inc=1, device_id={"ep": other}, device_id_type=MESH)

    if near:
        greet(barrier, 1)
        pl.when(inner == 1)(lambda: greet(barrier, 3))
        greeted = 3 + inner
    else:
        for k in range(1, groups):
            greet(barrier, k)
        greeted = 2 + groups - 1

    load_ids = pltpu.make_async_copy(ids_hbm, ids_row, w_sem.at[2])
    load_gates = pltpu.make_async_copy(gates_hbm, gates, w_sem.at[3])
    load_tokens = pltpu.make_async_copy(tokens_hbm, tokens, w_sem.at[4])
    load_in = pltpu.make_async_copy(weight_in, w_in, w_sem.at[0])
    load_out = pltpu.make_async_copy(weight_out, w_out, w_sem.at[1])
    for load in (load_ids, load_gates, load_tokens, load_in, load_out):
        load.start()

    lanes_e = -(-groups // 16) * 16
    t0 = lax.broadcasted_iota(jnp.int32, (tok_rows, tok_rows), 0)
    t1 = lax.broadcasted_iota(jnp.int32, (tok_rows, tok_rows), 1)
    load_ids.wait()
    ids = ids_row[...]
    hot = (lax.broadcasted_iota(jnp.int32, (lanes_e, tok_rows), 0) == ids).astype(F32)
    ahead = jnp.dot(hot.astype(BF16), (t0 < t1).astype(F32).astype(BF16), preferred_element_type=F32)
    slot = ids * seats + jnp.sum(hot * ahead, axis=0, keepdims=True).astype(jnp.int32)
    load_gates.wait()
    slot_c = jnp.sum(jnp.where(t0 == t1, slot, 0), axis=1, keepdims=True)
    weight = jnp.sum(jnp.where(t0 == t1, gates[...], 0.0), axis=1, keepdims=True)
    load_tokens.wait()

    def take(target, dst):
        seat = lax.broadcasted_iota(jnp.int32, (seats, tok_rows), 0) + target * seats
        place = (seat == slot).astype(F32).astype(BF16)
        for c in range(0, width, STEP):
            rows = jnp.dot(place, tokens[:, c : c + STEP], preferred_element_type=F32)
            dst[:, c : c + STEP] = rows.astype(BF16)

    def remote(src, dst, s_sem, r_sem, dev):
        return pltpu.make_async_remote_copy(
            src_ref=src,
            dst_ref=dst,
            send_sem=s_sem,
            recv_sem=r_sem,
            device_id={"ep": dev},
            device_id_type=MESH,
        )

    def drain(ref, sem):
        pltpu.make_async_copy(ref, ref, sem).wait()

    def seat_rows(ref, i):
        return ref.at[pl.ds(i * seats, seats)] if per > 1 else ref

    def run(order):
        members = [(p, i) for p in range(chunks) for i in range(per)][1:]
        spread, forward, early, late, z_copies, back = {}, {}, {}, {}, {}, {}

        def take_for(p, i):
            k = chunk_of[p] * per + i
            target = flip(group, k, groups)
            source = send.at[p * per + i]
            landing = seat_rows(gathered.at[chunk_of[p], lane], i)
            take(target, source)
            z_copies[p, i] = [
                remote(
                    source.at[:, cols],
                    landing.at[:, cols],
                    z_send,
                    z_recv.at[k - 1, h],
                    target * SLICES + lane,
                )
                for h, cols in enumerate(halves)
            ]

        def stage_t(p):
            if per == 1:
                take_for(p, 0)

        def leave(p):
            for i in range(per):
                if (p, i) in z_copies:
                    for copy in z_copies[p, i]:
                        copy.start()

        def stage_z(p):
            leave(p)

        def stage_n(p):
            pl.when(inner == 1)(lambda: leave(p))

        def stage_o(p):
            pl.when(inner == 0)(lambda: leave(p))

        def stage_u(p):
            if near and p == 2:
                pl.semaphore_wait(far_sem.at[0], 1)
                pl.when(inner == 1)(lambda: greet(far_sem.at[1], 1))
            if near and p == 3:
                pl.when(inner == 0)(lambda: pl.semaphore_wait(far_sem.at[1], 1))

        def stage_a(p):
            own = [gathered.at[chunk_of[p], lane, :, cols] for cols in halves]

            def arrive(h):
                for i in range(per):
                    if (p, i) in z_copies:
                        z_copies[p, i][h].wait_recv()

            spread[p] = [
                remote(own[h], own[h], g_send, g_recv.at[p, n], dev)
                for n, h, dev in ((0, 0, x_dev), (1, 1, y_dev), (2, 1, x_dev), (2, 0, y_dev))
            ]
            first = gathered.at[chunk_of[p], x_lane, :, halves[0]]
            second = gathered.at[chunk_of[p], y_lane, :, halves[1]]
            forward[p] = [
                remote(first, first, g_send, g_recv.at[p, 2], y_dev),
                remote(second, second, g_send, g_recv.at[p, 2], x_dev),
            ]
            arrive(0)
            spread[p][0].start()
            arrive(1)
            spread[p][1].start()

        def stage_c(p):
            for copy in spread[p][2:]:
                copy.start()

        def stage_b(p):
            spread[p][0].wait_recv()
            forward[p][0].start()

        def stage_k(p):
            spread[p][1].wait_recv()
            forward[p][1].start()

        rows = per * seats
        tile = STEP

        def stage_g(p):
            drain(gathered.at[chunk_of[p], pl.ds(0, 2)], g_recv.at[p, 2])
            staged[...] = stack_rows([gathered[chunk_of[p], s] for s in range(SLICES)])
            if p == 0:
                load_in.wait()

            @pl.loop(0, w_in.shape[1] // tile)
            def _(n):
                cols = pl.ds(pl.multiple_of(n * tile, tile), tile)
                value = jnp.dot(staged[...], w_in[:, cols], preferred_element_type=F32)
                hidden[:, cols] = jnp.maximum(value, 0.0).astype(BF16)

            if p == 0:
                load_out.wait()

        def project(p, start):
            @pl.loop(0, half // tile)
            def _(n):
                cols = pl.ds(pl.multiple_of(start + n * tile, tile), tile)
                value = jnp.dot(hidden[...], w_out[:, cols], preferred_element_type=F32)
                for s in range(SLICES):
                    parts[p, s, :, cols] = value[s * rows : (s + 1) * rows].astype(BF16)

        def stage_p(p):
            project(p, 0)

        def stage_q(p):
            project(p, half)

        def to(p, n, src, dst, dev):
            return remote(src, dst, r_send, r_recv.at[p, n], dev)

        def stage_y(p):
            early[p, 0] = to(p, 0, parts.at[p, d_lane, :, halves[0]], diag_a.at[p], y_dev)
            early[p, 0].start()

        def stage_w(p):
            early[p, 1] = to(
                p, 2, parts.at[p, y_lane, :, halves[0]], from_y.at[p, :, halves[0]], y_dev
            )
            early[p, 1].start()

        def stage_x(p):
            early[p, 2] = to(p, 1, parts.at[p, d_lane, :, halves[1]], diag_b.at[p], x_dev)
            early[p, 2].start()

        def stage_v(p):
            early[p, 3] = to(
                p, 3, parts.at[p, x_lane, :, halves[1]], from_x.at[p, :, halves[1]], x_dev
            )
            early[p, 3].start()

        def stage_e(p):
            late[p, 0] = to(p, 2, parts.at[p, x_lane, :, halves[0]], from_x.at[p, :, halves[0]], x_dev)
            early[p, 0].wait_recv()
            parts[p, x_lane, :, :half] = (
                parts[p, x_lane, :, :half].astype(F32) + diag_a[p].astype(F32)
            ).astype(BF16)
            late[p, 0].start()

        def stage_h(p):
            late[p, 1] = to(p, 3, parts.at[p, y_lane, :, halves[1]], from_y.at[p, :, halves[1]], y_dev)
            early[p, 2].wait_recv()
            parts[p, y_lane, :, half:] = (
                parts[p, y_lane, :, half:].astype(F32) + diag_b[p].astype(F32)
            ).astype(BF16)
            late[p, 1].start()

        def finish(p, h):
            cols = slice(h * half, (h + 1) * half)
            drain(from_x.at[p], r_recv.at[p, 2 + h])
            sums[p, :, cols] = (
                parts[p, lane, :, cols].astype(F32)
                + from_x[p, :, cols].astype(F32)
                + from_y[p, :, cols].astype(F32)
            ).astype(BF16)
            for i in range(per):
                if (p, i) in z_copies:
                    k = chunk_of[p] * per + i
                    back[p, i, h] = remote(
                        seat_rows(sums.at[p], i).at[:, halves[h]],
                        returned.at[k, :, halves[h]],
                        b_send,
                        b_recv.at[chunk_of[p]],
                        flip(group, k, groups) * SLICES + lane,
                    )
                    back[p, i, h].start()

        def stage_f(p):
            finish(p, 0)

        def stage_i(p):
            finish(p, 1)

        def picks_of(wanted):
            picks = []
            for p, i in wanted:
                target = flip(group, chunk_of[p] * per + i, groups)
                seat = lax.broadcasted_iota(jnp.int32, (tok_rows, seats), 1) + target * seats
                picks.append((seat == slot_c).astype(F32))
            return jnp.concatenate(picks, axis=1).astype(BF16)

        def gather(wanted, c):
            blocks = []
            for q, i in wanted:
                if (q, i) == (0, 0):
                    blocks.append(sums[0, :seats, c : c + STEP])
                else:
                    blocks.append(returned[chunk_of[q] * per + i, :, c : c + STEP])
            return jnp.dot(picks_of(wanted), stack_rows(blocks), preferred_element_type=F32)

        def returns(p):
            count = per - 1 if p == 0 else per
            if count:
                drain(returned.at[pl.ds(0, count)], b_recv.at[chunk_of[p]])
            return [(p, i) for i in range(per)]

        def stage_r(p):
            wanted = returns(p)
            for c in range(0, width, STEP):
                total[:, c : c + STEP] = gather(wanted, c)

        def stage_s(p):
            wanted = returns(0) + returns(p)
            for c in range(0, width, STEP):
                total[:, c : c + STEP] += gather(wanted, c)

        def stage_j(p):
            wanted = returns(p)
            for c in range(0, width, STEP):
                picked = total[:, c : c + STEP] + gather(wanted, c)
                out[:, c : c + STEP] = (weight * picked).astype(BF16)

        take(group, seat_rows(gathered.at[0, lane], 0))
        if per > 1:
            for p, i in members:
                take_for(p, i)
        pl.semaphore_wait(barrier, greeted)
        if near:

            @pl.when(inner == 1)
            def _():
                greet(far_sem.at[0], 1)
                greet(far_sem.at[0], 3)

        if per > 1:
            leave(0)

        stages = {
            "a": stage_a,
            "c": stage_c,
            "t": stage_t,
            "u": stage_u,
            "Z": stage_z,
            "N": stage_n,
            "O": stage_o,
            "B": stage_b,
            "C": stage_k,
            "G": stage_g,
            "P": stage_p,
            "Q": stage_q,
            "y": stage_y,
            "w": stage_w,
            "x": stage_x,
            "v": stage_v,
            "E": stage_e,
            "H": stage_h,
            "F": stage_f,
            "I": stage_i,
            "R": stage_r,
            "S": stage_s,
            "T": stage_j,
        }
        for name, p in zip(order[::2], order[1::2]):
            stages[name](int(p))

        drain(send.at[pl.ds(0, len(members))], z_send)
        drain(parts.at[pl.ds(0, 3)], g_send)
        drain(parts.at[pl.ds(0, 3)], r_send)
        drain(returned.at[pl.ds(0, len(members))], b_send)

    if ORDER == OTHER:
        run("".join(ORDER))
    else:
        core = lax.axis_index("rep")
        pl.when(core == 0)(lambda: run("".join(ORDER)))
        pl.when(core != 0)(lambda: run("".join(OTHER)))


def body(tokens, gates, expert_ids, weight_in, weight_out):
    owner_count = lax.axis_size("ep")
    tok_rows, width = tokens.shape
    groups, chunks, per, seats = layout(owner_count, tok_rows)
    rows = per * seats
    half = width // 2
    hbm = pl.BlockSpec(memory_space=pltpu.HBM)
    dma = pltpu.SemaphoreType.DMA
    return pl.pallas_call(
        functools.partial(kernel, owner_count),
        out_shape=jax.ShapeDtypeStruct((tok_rows, width), BF16),
        in_specs=[hbm] * 5,
        out_specs=pl.BlockSpec(memory_space=pltpu.VMEM),
        scratch_shapes=[
            pltpu.VMEM((1, tok_rows), jnp.int32),
            pltpu.VMEM((1, tok_rows), F32),
            pltpu.VMEM((tok_rows, width), BF16),
            pltpu.VMEM(weight_in.shape, BF16),
            pltpu.VMEM(weight_out.shape, BF16),
            pltpu.VMEM((groups, seats, width), BF16),
            pltpu.VMEM((chunks, SLICES, rows, width), BF16),
            pltpu.VMEM((SLICES * rows, width), BF16),
            pltpu.VMEM((SLICES * rows, weight_in.shape[1]), BF16),
            pltpu.VMEM((chunks, SLICES, rows, width), BF16),
            pltpu.VMEM((chunks, rows, half), BF16),
            pltpu.VMEM((chunks, rows, half), BF16),
            pltpu.VMEM((chunks, rows, width), BF16),
            pltpu.VMEM((chunks, rows, width), BF16),
            pltpu.VMEM((chunks, rows, width), BF16),
            pltpu.VMEM((groups, seats, width), BF16),
            pltpu.VMEM((tok_rows, width), F32),
            dma((5,)),
            dma,
            dma((groups - 1, 2)),
            dma,
            dma((chunks, 3)),
            dma,
            dma((chunks, 4)),
            dma,
            dma((chunks,)),
            pltpu.SemaphoreType.REGULAR((2,)),
        ],
        compiler_params=pltpu.CompilerParams(
            collective_id=0, has_side_effects=True, vmem_limit_bytes=48 * 1024 * 1024
        ),
    )(
        *(
            pltpu.with_memory_space_constraint(array, pltpu.HBM)
            for array in (
                expert_ids.reshape(1, tok_rows),
                gates.reshape(1, tok_rows),
                tokens,
                weight_in,
                weight_out,
            )
        )
    )


def solution(mesh):
    in_specs = (
        P(("rep", "ep"), None),
        P(("rep", "ep")),
        P(("rep", "ep"), None),
        P(None, "ep"),
        P("ep", None),
    )
    out_specs = P(("rep", "ep"), None)
    return jax.shard_map(body, mesh=mesh, in_specs=in_specs, out_specs=out_specs, check_vma=False)
```

```python
import functools

import jax
import jax.numpy as jnp
from jax import lax
from jax.experimental import pallas as pl
from jax.experimental.pallas import tpu as pltpu
from jax.sharding import PartitionSpec as P

SLICES = 4
CHUNKS = 4
STEP = 512
ORDER = (
    "a0c0t1Z1t2N2C0B0t3u2N3a1c1G0B1C1u3O3P0O2a2Q0c2G1P1C2B2Q1a3c3",
    "G2x1w1P2C3B3y1Q2x2G3P3E1v2y3Q3x3H2y2E3w3H3w2v3F1I2E2x0y0v1F3",
    "H1v0I3F2H0w0E0I1R3F0I0S2T1",
)
OTHER = ORDER
BF16 = jnp.bfloat16
F32 = jnp.float32
MESH = pl.DeviceIdType.MESH


def layout(owner_count, tok_rows):
    groups = owner_count // SLICES
    chunks = CHUNKS
    per = groups // chunks
    seats = 3 * tok_rows // (4 * groups) + tok_rows // (2 * groups)
    unit = 8 if per == 1 else 16
    seats = -(-seats // unit) * unit
    return groups, chunks, per, seats


def stack_rows(blocks):
    return jnp.concatenate([block.astype(F32) for block in blocks], axis=0).astype(BF16)


def flip(a, b, count):
    total, bit = 0, 1
    while bit < count:
        total = total + (a // bit % 2 + b // bit % 2) % 2 * bit
        bit *= 2
    return total


def kernel(
    owner_count,
    ids_hbm,
    gates_hbm,
    tokens_hbm,
    weight_in,
    weight_out,
    out,
    ids_row,
    gates,
    tokens,
    w_in,
    w_out,
    send,
    gathered,
    staged,
    hidden,
    parts,
    diag_a,
    diag_b,
    from_x,
    from_y,
    sums,
    returned,
    total,
    w_sem,
    z_send,
    z_recv,
    g_send,
    g_recv,
    r_send,
    r_recv,
    b_send,
    b_recv,
    far_sem,
):
    tok_rows, width = tokens.shape
    groups, chunks, per, seats = layout(owner_count, tok_rows)
    half = width // 2
    halves = (pl.ds(0, half), pl.ds(half, half))
    me = lax.axis_index("ep")
    group = me // SLICES
    lane = me % SLICES
    x_bit, y_bit = lane % 2, lane // 2
    x_lane = y_bit * 2 + (1 - x_bit)
    y_lane = (1 - y_bit) * 2 + x_bit
    d_lane = (1 - y_bit) * 2 + (1 - x_bit)
    x_dev = group * SLICES + x_lane
    y_dev = group * SLICES + y_lane
    inner = (group % 2 + group // 2 % 2) % 2
    chunk_of = [0, 1, 2 + inner, 3 - inner]

    barrier = pltpu.get_barrier_semaphore()
    pl.semaphore_signal(barrier, inc=1, device_id={"ep": x_dev}, device_id_type=MESH)
    pl.semaphore_signal(barrier, inc=1, device_id={"ep": y_dev}, device_id_type=MESH)
    near = groups == 4

    def greet(sem, k):
        other = flip(group, k, groups) * SLICES + lane
        pl.semaphore_signal(sem, inc=1, device_id={"ep": other}, device_id_type=MESH)

    if near:
        greet(barrier, 1)
        pl.when(inner == 1)(lambda: greet(barrier, 3))
        greeted = 3 + inner
    else:
        for k in range(1, groups):
            greet(barrier, k)
        greeted = 2 + groups - 1

    load_ids = pltpu.make_async_copy(ids_hbm, ids_row, w_sem.at[2])
    load_gates = pltpu.make_async_copy(gates_hbm, gates, w_sem.at[3])
    load_tokens = pltpu.make_async_copy(tokens_hbm, tokens, w_sem.at[4])
    load_in = pltpu.make_async_copy(weight_in, w_in, w_sem.at[0])
    load_out = pltpu.make_async_copy(weight_out, w_out, w_sem.at[1])
    for load in (load_ids, load_gates, load_tokens, load_in, load_out):
        load.start()

    lanes_e = -(-groups // 16) * 16
    t0 = lax.broadcasted_iota(jnp.int32, (tok_rows, tok_rows), 0)
    t1 = lax.broadcasted_iota(jnp.int32, (tok_rows, tok_rows), 1)
    load_ids.wait()
    ids = ids_row[...]
    hot = (lax.broadcasted_iota(jnp.int32, (lanes_e, tok_rows), 0) == ids).astype(F32)
    ahead = jnp.dot(hot.astype(BF16), (t0 < t1).astype(F32).astype(BF16), preferred_element_type=F32)
    slot = ids * seats + jnp.sum(hot * ahead, axis=0, keepdims=True).astype(jnp.int32)
    load_gates.wait()
    slot_c = jnp.sum(jnp.where(t0 == t1, slot, 0), axis=1, keepdims=True)
    weight = jnp.sum(jnp.where(t0 == t1, gates[...], 0.0), axis=1, keepdims=True)
    load_tokens.wait()

    def take(target, dst):
        seat = lax.broadcasted_iota(jnp.int32, (seats, tok_rows), 0) + target * seats
        place = (seat == slot).astype(F32).astype(BF16)
        for c in range(0, width, STEP):
            rows = jnp.dot(place, tokens[:, c : c + STEP], preferred_element_type=F32)
            dst[:, c : c + STEP] = rows.astype(BF16)

    def remote(src, dst, s_sem, r_sem, dev):
        return pltpu.make_async_remote_copy(
            src_ref=src,
            dst_ref=dst,
            send_sem=s_sem,
            recv_sem=r_sem,
            device_id={"ep": dev},
            device_id_type=MESH,
        )

    def drain(ref, sem):
        pltpu.make_async_copy(ref, ref, sem).wait()

    def seat_rows(ref, i):
        return ref.at[pl.ds(i * seats, seats)] if per > 1 else ref

    def run(order):
        members = [(p, i) for p in range(chunks) for i in range(per)][1:]
        spread, forward, early, late, z_copies, back = {}, {}, {}, {}, {}, {}

        def take_for(p, i):
            k = chunk_of[p] * per + i
            target = flip(group, k, groups)
            source = send.at[p * per + i]
            landing = seat_rows(gathered.at[chunk_of[p], lane], i)
            take(target, source)
            z_copies[p, i] = [
                remote(
                    source.at[:, cols],
                    landing.at[:, cols],
                    z_send,
                    z_recv.at[k - 1, h],
                    target * SLICES + lane,
                )
                for h, cols in enumerate(halves)
            ]

        def stage_t(p):
            if per == 1:
                take_for(p, 0)

        def leave(p):
            for i in range(per):
                if (p, i) in z_copies:
                    for copy in z_copies[p, i]:
                        copy.start()

        def stage_z(p):
            leave(p)

        def stage_n(p):
            pl.when(inner == 1)(lambda: leave(p))

        def stage_o(p):
            pl.when(inner == 0)(lambda: leave(p))

        def stage_u(p):
            if near and p == 2:
                pl.semaphore_wait(far_sem.at[0], 1)
                pl.when(inner == 1)(lambda: greet(far_sem.at[1], 1))
            if near and p == 3:
                pl.when(inner == 0)(lambda: pl.semaphore_wait(far_sem.at[1], 1))

        def stage_a(p):
            own = [gathered.at[chunk_of[p], lane, :, cols] for cols in halves]

            def arrive(h):
                for i in range(per):
                    if (p, i) in z_copies:
                        z_copies[p, i][h].wait_recv()

            spread[p] = [
                remote(own[h], own[h], g_send, g_recv.at[p, n], dev)
                for n, h, dev in ((0, 0, x_dev), (1, 1, y_dev), (2, 1, x_dev), (2, 0, y_dev))
            ]
            first = gathered.at[chunk_of[p], x_lane, :, halves[0]]
            second = gathered.at[chunk_of[p], y_lane, :, halves[1]]
            forward[p] = [
                remote(first, first, g_send, g_recv.at[p, 2], y_dev),
                remote(second, second, g_send, g_recv.at[p, 2], x_dev),
            ]
            arrive(0)
            spread[p][0].start()
            arrive(1)
            spread[p][1].start()

        def stage_c(p):
            for copy in spread[p][2:]:
                copy.start()

        def stage_b(p):
            spread[p][0].wait_recv()
            forward[p][0].start()

        def stage_k(p):
            spread[p][1].wait_recv()
            forward[p][1].start()

        rows = per * seats
        tile = STEP

        def stage_g(p):
            drain(gathered.at[chunk_of[p], pl.ds(0, 2)], g_recv.at[p, 2])
            staged[...] = stack_rows([gathered[chunk_of[p], s] for s in range(SLICES)])
            if p == 0:
                load_in.wait()

            @pl.loop(0, w_in.shape[1] // tile)
            def _(n):
                cols = pl.ds(pl.multiple_of(n * tile, tile), tile)
                value = jnp.dot(staged[...], w_in[:, cols], preferred_element_type=F32)
                hidden[:, cols] = jnp.maximum(value, 0.0).astype(BF16)

            if p == 0:
                load_out.wait()

        def project(p, start):
            @pl.loop(0, half // tile)
            def _(n):
                cols = pl.ds(pl.multiple_of(start + n * tile, tile), tile)
                value = jnp.dot(hidden[...], w_out[:, cols], preferred_element_type=F32)
                for s in range(SLICES):
                    parts[p, s, :, cols] = value[s * rows : (s + 1) * rows].astype(BF16)

        def stage_p(p):
            project(p, 0)

        def stage_q(p):
            project(p, half)

        def to(p, n, src, dst, dev):
            return remote(src, dst, r_send, r_recv.at[p, n], dev)

        def stage_y(p):
            early[p, 0] = to(p, 0, parts.at[p, d_lane, :, halves[0]], diag_a.at[p], y_dev)
            early[p, 0].start()

        def stage_w(p):
            early[p, 1] = to(
                p, 2, parts.at[p, y_lane, :, halves[0]], from_y.at[p, :, halves[0]], y_dev
            )
            early[p, 1].start()

        def stage_x(p):
            early[p, 2] = to(p, 1, parts.at[p, d_lane, :, halves[1]], diag_b.at[p], x_dev)
            early[p, 2].start()

        def stage_v(p):
            early[p, 3] = to(
                p, 3, parts.at[p, x_lane, :, halves[1]], from_x.at[p, :, halves[1]], x_dev
            )
            early[p, 3].start()

        def stage_e(p):
            late[p, 0] = to(p, 2, parts.at[p, x_lane, :, halves[0]], from_x.at[p, :, halves[0]], x_dev)
            early[p, 0].wait_recv()
            parts[p, x_lane, :, :half] = (
                parts[p, x_lane, :, :half].astype(F32) + diag_a[p].astype(F32)
            ).astype(BF16)
            late[p, 0].start()

        def stage_h(p):
            late[p, 1] = to(p, 3, parts.at[p, y_lane, :, halves[1]], from_y.at[p, :, halves[1]], y_dev)
            early[p, 2].wait_recv()
            parts[p, y_lane, :, half:] = (
                parts[p, y_lane, :, half:].astype(F32) + diag_b[p].astype(F32)
            ).astype(BF16)
            late[p, 1].start()

        def finish(p, h):
            cols = slice(h * half, (h + 1) * half)
            drain(from_x.at[p], r_recv.at[p, 2 + h])
            sums[p, :, cols] = (
                parts[p, lane, :, cols].astype(F32)
                + from_x[p, :, cols].astype(F32)
                + from_y[p, :, cols].astype(F32)
            ).astype(BF16)
            for i in range(per):
                if (p, i) in z_copies:
                    k = chunk_of[p] * per + i
                    back[p, i, h] = remote(
                        seat_rows(sums.at[p], i).at[:, halves[h]],
                        returned.at[k, :, halves[h]],
                        b_send,
                        b_recv.at[chunk_of[p]],
                        flip(group, k, groups) * SLICES + lane,
                    )
                    back[p, i, h].start()

        def stage_f(p):
            finish(p, 0)

        def stage_i(p):
            finish(p, 1)

        def picks_of(wanted):
            picks = []
            for p, i in wanted:
                target = flip(group, chunk_of[p] * per + i, groups)
                seat = lax.broadcasted_iota(jnp.int32, (tok_rows, seats), 1) + target * seats
                picks.append((seat == slot_c).astype(F32))
            return jnp.concatenate(picks, axis=1).astype(BF16)

        def gather(pick, wanted, c):
            blocks = []
            for q, i in wanted:
                if (q, i) == (0, 0):
                    blocks.append(sums[0, :seats, c : c + STEP])
                else:
                    blocks.append(returned[chunk_of[q] * per + i, :, c : c + STEP])
            return jnp.dot(pick, stack_rows(blocks), preferred_element_type=F32)

        def returns(p):
            count = per - 1 if p == 0 else per
            if count:
                drain(returned.at[pl.ds(0, count)], b_recv.at[chunk_of[p]])

        def rows_of(p):
            return [(p, i) for i in range(per)]

        def stage_r(p):
            wanted = rows_of(p)
            pick = picks_of(wanted)
            returns(p)
            for c in range(0, width, STEP):
                total[:, c : c + STEP] = gather(pick, wanted, c)

        def stage_s(p):
            wanted = rows_of(0) + rows_of(p)
            pick = picks_of(wanted)
            returns(0)
            returns(p)
            for c in range(0, width, STEP):
                total[:, c : c + STEP] += gather(pick, wanted, c)

        def stage_j(p):
            wanted = rows_of(p)
            pick = picks_of(wanted)
            returns(p)
            for c in range(0, width, STEP):
                picked = total[:, c : c + STEP] + gather(pick, wanted, c)
                out[:, c : c + STEP] = (weight * picked).astype(BF16)

        take(group, seat_rows(gathered.at[0, lane], 0))
        if per > 1:
            for p, i in members:
                take_for(p, i)
        pl.semaphore_wait(barrier, greeted)
        if near:

            @pl.when(inner == 1)
            def _():
                greet(far_sem.at[0], 1)
                greet(far_sem.at[0], 3)

        if per > 1:
            leave(0)

        stages = {
            "a": stage_a,
            "c": stage_c,
            "t": stage_t,
            "u": stage_u,
            "Z": stage_z,
            "N": stage_n,
            "O": stage_o,
            "B": stage_b,
            "C": stage_k,
            "G": stage_g,
            "P": stage_p,
            "Q": stage_q,
            "y": stage_y,
            "w": stage_w,
            "x": stage_x,
            "v": stage_v,
            "E": stage_e,
            "H": stage_h,
            "F": stage_f,
            "I": stage_i,
            "R": stage_r,
            "S": stage_s,
            "T": stage_j,
        }
        for name, p in zip(order[::2], order[1::2]):
            stages[name](int(p))

        drain(send.at[pl.ds(0, len(members))], z_send)
        drain(parts.at[pl.ds(0, 3)], g_send)
        drain(parts.at[pl.ds(0, 3)], r_send)
        drain(returned.at[pl.ds(0, len(members))], b_send)

    if ORDER == OTHER:
        run("".join(ORDER))
    else:
        core = lax.axis_index("rep")
        pl.when(core == 0)(lambda: run("".join(ORDER)))
        pl.when(core != 0)(lambda: run("".join(OTHER)))


def body(tokens, gates, expert_ids, weight_in, weight_out):
    owner_count = lax.axis_size("ep")
    tok_rows, width = tokens.shape
    groups, chunks, per, seats = layout(owner_count, tok_rows)
    rows = per * seats
    half = width // 2
    hbm = pl.BlockSpec(memory_space=pltpu.HBM)
    dma = pltpu.SemaphoreType.DMA
    return pl.pallas_call(
        functools.partial(kernel, owner_count),
        out_shape=jax.ShapeDtypeStruct((tok_rows, width), BF16),
        in_specs=[hbm] * 5,
        out_specs=pl.BlockSpec(memory_space=pltpu.VMEM),
        scratch_shapes=[
            pltpu.VMEM((1, tok_rows), jnp.int32),
            pltpu.VMEM((1, tok_rows), F32),
            pltpu.VMEM((tok_rows, width), BF16),
            pltpu.VMEM(weight_in.shape, BF16),
            pltpu.VMEM(weight_out.shape, BF16),
            pltpu.VMEM((groups, seats, width), BF16),
            pltpu.VMEM((chunks, SLICES, rows, width), BF16),
            pltpu.VMEM((SLICES * rows, width), BF16),
            pltpu.VMEM((SLICES * rows, weight_in.shape[1]), BF16),
            pltpu.VMEM((chunks, SLICES, rows, width), BF16),
            pltpu.VMEM((chunks, rows, half), BF16),
            pltpu.VMEM((chunks, rows, half), BF16),
            pltpu.VMEM((chunks, rows, width), BF16),
            pltpu.VMEM((chunks, rows, width), BF16),
            pltpu.VMEM((chunks, rows, width), BF16),
            pltpu.VMEM((groups, seats, width), BF16),
            pltpu.VMEM((tok_rows, width), F32),
            dma((5,)),
            dma,
            dma((groups - 1, 2)),
            dma,
            dma((chunks, 3)),
            dma,
            dma((chunks, 4)),
            dma,
            dma((chunks,)),
            pltpu.SemaphoreType.REGULAR((2,)),
        ],
        compiler_params=pltpu.CompilerParams(
            collective_id=0, has_side_effects=True, vmem_limit_bytes=48 * 1024 * 1024
        ),
    )(
        *(
            pltpu.with_memory_space_constraint(array, pltpu.HBM)
            for array in (
                expert_ids.reshape(1, tok_rows),
                gates.reshape(1, tok_rows),
                tokens,
                weight_in,
                weight_out,
            )
        )
    )


def solution(mesh):
    in_specs = (
        P(("rep", "ep"), None),
        P(("rep", "ep")),
        P(("rep", "ep"), None),
        P(None, "ep"),
        P("ep", None),
    )
    out_specs = P(("rep", "ep"), None)
    return jax.shard_map(body, mesh=mesh, in_specs=in_specs, out_specs=out_specs, check_vma=False)
```
